32 devices in a mesh: ep: 16 (over z, y, x), tp: 2 (over core).
Axes of the slice: x: 2, y: 2, z: 4, core: 2. Of those that a mesh axis runs over, the one named last changes fastest.
Arguments:
- tokens: bfloat16 [2048, 3584], P('ep'), may hold values from -6 to 6
- expert_ids: int32 [2048, 8], P('ep'), may hold values from 0 to 15, all different within a row; in each aligned block of 128 rows (0 to 127, 128 to 255, ...) at most 96 rows name the same one
- gate_values: float32 [2048, 8], P('ep'), may hold values from 0.05 to 1
- w_gate: bfloat16 [16, 3584, 1024], P('ep', None, 'tp'), may hold values from -0.09375 to 0.09375
- w_up: bfloat16 [16, 3584, 1024], P('ep', None, 'tp'), may hold values from -0.09375 to 0.09375
- w_down: bfloat16 [16, 1024, 3584], P('ep', 'tp'), may hold values from -0.1875 to 0.1875
- shared_gate: bfloat16 [3584, 1024], P(None, 'tp'), may hold values from -0.09375 to 0.09375
- shared_up: bfloat16 [3584, 1024], P(None, 'tp'), may hold values from -0.09375 to 0.09375
- shared_down: bfloat16 [1024, 3584], P('tp'), may hold values from -0.1875 to 0.1875
Outputs:
- layer_out: bfloat16 [2048, 3584], P('ep', 'tp')
The draws below stay inside these ranges and needn't reach their ends.
Inputs may be any that keep to these rules, and one draw needn't show every extreme that they name: `expert_ids`: each row names 8 different experts; within the rows of one index of ep (aligned blocks of 128 rows) no expert is named by more than 96 rows.
All inputs are finite; a program needn't handle non-finite values.
Results may differ from the reference program's by a relative error of at most 0.0085.
Values may be sent and summed in bfloat16 or wider, within the bound.
A program may use at most 128 MiB of HBM per device.

```python
import math
import jax
import jax.numpy as jnp
import numpy as np
from jax import lax

D = 3584
FE = 1024
FS = 1024
TOPK = 8
TOK_DEV = 128
EXPERTS = 16
TOKENS = 2048
CAP = 96
N_EP = 16


def levels(key, extent, cuts, low, top_value):
    level, own = 1.0, jax.random.fold_in(key, 6)
    for position, shards_of in cuts:
        steps = jnp.exp(jax.random.uniform(jax.random.fold_in(own, position), (shards_of,), jnp.float32, low / len(cuts), top_value / len(cuts)))
        level = level * jnp.repeat(steps, extent[position] // shards_of).reshape([-1 if axis == position else 1 for axis in range(len(extent))])
    return level


def routed_block(key, own, number, rows, count, top, reach, slope):
    order = jax.random.permutation(key, count)
    crowded, ordinary = shares(count, rows * top, reach, slope, True), shares(count, rows * top, reach, slope, False)
    places = jnp.arange(count)

    def named(tallies, turn):
        used = int((tallies > 0).sum())
        fixed = max(1, used // 4)
        shifted = fixed + (places - fixed + turn * (used - fixed)) % max(1, count - fixed)
        return jnp.zeros((count,), jnp.int32).at[order[jnp.where(places < fixed, places, shifted)]].set(jnp.asarray(tallies, jnp.int32))

    tallies = jnp.where(number % 4 == 0, named(crowded, number // 4), named(ordinary, number - number // 4 - 1))
    mixed = jax.random.permutation(jax.random.fold_in(own, 3), count)
    donor, receiver = mixed[0:count // 2 * 2:2], mixed[1:count // 2 * 2:2]
    margin = jnp.minimum(tallies[donor] - 1, reach - tallies[receiver]) // 2
    margin = jnp.where((donor == order[0]) | (receiver == order[0]) | (tallies[receiver] == 0), 0, jnp.maximum(margin, 0))
    shifted = jax.random.randint(jax.random.fold_in(own, 4), (count // 2,), 0, 1 << 20) % (margin + 1)
    tallies = tallies.at[donor].add(-shifted).at[receiver].add(shifted)
    labels = jnp.searchsorted(jnp.cumsum(tallies), jnp.arange(rows * top), side="right").astype(jnp.int32)
    grid = labels.reshape(top, rows).T
    grid = grid[jax.random.permutation(jax.random.fold_in(own, 1), rows)]
    turn = jax.random.randint(jax.random.fold_in(own, 2), (rows, 1), 0, top)
    return jnp.take_along_axis(grid, (jnp.arange(top)[None, :] + turn) % top, axis=1)


def shares(count, total, reach, skew, full):
    weights = [(1 << 20) // math.isqrt(grade ** skew) + 1 for grade in range(1, count + 1)]
    largest = reach if full else min(reach, max(-(-total // count), total * weights[0] // sum(weights)))
    least = 1 if total - largest >= count - 1 else 0
    holding, surplus = [largest] + [least] * (count - 1), total - largest - least * (count - 1)
    while surplus > 0:
        free = [i for i in range(1, count) if holding[i] < largest] or [i for i in range(1, count) if holding[i] < reach]
        whole, budget = sum([weights[i] for i in free]), surplus
        for i in free:
            extra = min(reach - holding[i], max(1, budget * weights[i] // whole), surplus)
            holding[i] = holding[i] + extra
            surplus = surplus - extra
    return np.array(holding)


def normal_values(own_key, shape, spread, reach, pieces=(), kind=jnp.bfloat16):
    gain = levels(own_key, shape, pieces, -0.22, 0.18) if pieces else 1.0
    entries = jax.random.normal(own_key, shape, jnp.float32) * spread * gain
    return jnp.minimum(jnp.maximum(entries, -reach), reach).astype(kind)


def setup_inputs(seed: int = 0) -> dict:
    streams_of = jax.random.split(jax.random.key(seed), 10)
    tokens = normal_values(streams_of[0], (TOKENS, D), 1.0, 6.0, ((0, 16),))
    expert_ids_keys = jax.random.split(jax.random.fold_in(streams_of[1], 1), TOKENS // TOK_DEV)
    expert_ids_turns = jax.random.permutation(jax.random.fold_in(streams_of[1], 3), TOKENS // TOK_DEV)
    expert_ids = jax.vmap(lambda own, number: routed_block(jax.random.fold_in(streams_of[1], 2), own, number, TOK_DEV, EXPERTS, TOPK, CAP, 2))(expert_ids_keys, expert_ids_turns).reshape((TOKENS, TOPK))
    gate_values = jnp.clip(jnp.exp(math.log(1.0) - 2.9957323 * jax.random.uniform(streams_of[2], (TOKENS, TOPK), jnp.float32) ** levels(streams_of[2], (TOKENS, TOPK), ((0, 16),), -0.2, 0.2)), 0.05, 1.0)
    w_gate = normal_values(streams_of[3], (EXPERTS, D, FE), D ** -0.5, 0.09375, ((0, 16), (2, 2)))
    w_up = normal_values(streams_of[4], (EXPERTS, D, FE), D ** -0.5, 0.09375, ((0, 16), (2, 2)))
    w_down = normal_values(streams_of[5], (EXPERTS, FE, D), FE ** -0.5, 0.1875, ((0, 16), (1, 2)))
    shared_gate = normal_values(streams_of[6], (D, FS), D ** -0.5, 0.09375, ((1, 2),))
    shared_up = normal_values(streams_of[7], (D, FS), D ** -0.5, 0.09375, ((1, 2),))
    shared_down = normal_values(streams_of[8], (FS, D), FS ** -0.5, 0.1875, ((0, 2),))
    return {"tokens": tokens, "expert_ids": expert_ids, "gate_values": gate_values, "w_gate": w_gate, "w_up": w_up, "w_down": w_down, "shared_gate": shared_gate, "shared_up": shared_up, "shared_down": shared_down}


route_scale = 2.827


def expert_apply(inputs, gate_matrix, up_matrix, down_matrix):
    gate_out = jnp.dot(inputs, gate_matrix, preferred_element_type=jnp.float32)
    up_out = jnp.dot(inputs, up_matrix, preferred_element_type=jnp.float32)
    hidden = (jax.nn.silu(gate_out) * up_out).astype(jnp.bfloat16)
    return jnp.dot(hidden, down_matrix, preferred_element_type=jnp.float32)


def reference(tokens, expert_ids, gate_values, w_gate, w_up, w_down, shared_gate, shared_up, shared_down):
    weights = route_scale * gate_values / jnp.sum(gate_values, axis=1, keepdims=True)
    flat_ids = expert_ids.reshape(-1)
    flat_weights = jnp.concatenate([weights.reshape(-1), jnp.zeros((1,), jnp.float32)])
    padded = jnp.concatenate([tokens, jnp.zeros((1, D), jnp.bfloat16)], axis=0)
    row_limit = N_EP * CAP

    def add_expert(totals, inputs):
        gate_matrix, up_matrix, down_matrix, expert = inputs
        positions = jnp.nonzero(flat_ids == expert, size=row_limit, fill_value=TOKENS * TOPK)[0].astype(jnp.int32)
        token_idx = (positions // TOPK).astype(jnp.int32)
        result = expert_apply(padded[token_idx], gate_matrix, up_matrix, down_matrix)
        result = result * flat_weights[positions][:, None]
        return totals.at[token_idx].add(result, mode="drop"), None

    start = jnp.zeros((TOKENS, D), jnp.float32)
    routed, _ = lax.scan(add_expert, start, (w_gate, w_up, w_down, jnp.arange(EXPERTS, dtype=jnp.int32)))
    shared = expert_apply(tokens, shared_gate, shared_up, shared_down)
    return (routed + shared).astype(jnp.bfloat16)
```

```python
import functools
import math

import jax
import jax.numpy as jnp
from jax import lax
from jax.experimental import pallas as pl
from jax.experimental.pallas import tpu as pltpu
from jax.sharding import PartitionSpec as P

route_scale = 2.827


def expert_apply(inputs, gate_matrix, up_matrix, down_matrix):
    gate_out = jnp.dot(inputs, gate_matrix, preferred_element_type=jnp.float32)
    up_out = jnp.dot(inputs, up_matrix, preferred_element_type=jnp.float32)
    hidden = (jax.nn.silu(gate_out) * up_out).astype(jnp.bfloat16)
    return jnp.dot(hidden, down_matrix, preferred_element_type=jnp.float32)


def combine_rows(returned, target, weights, tok_rows, top_count):
    feature_count = returned.shape[-1]
    picked = jnp.take(returned.reshape(-1, feature_count), target, axis=0)
    picked = picked.reshape(tok_rows, top_count, feature_count)
    return jnp.sum(picked * weights[:, :, None], axis=1)


def per_device_routed(
    tokens, expert_ids, gate_values, w_gate, w_up, w_down, shared_gate, shared_up, shared_down
):
    ep_count = lax.axis_size("ep")
    tp_count = lax.axis_size("tp")
    tok_rows, model_width = tokens.shape
    top_count = expert_ids.shape[1]
    experts = ep_count * w_gate.shape[0]
    capacity = 3 * tok_rows * top_count // (2 * experts)
    weights = route_scale * gate_values / jnp.sum(gate_values, axis=1, keepdims=True)
    flat_ids = expert_ids.reshape(-1)
    onehot = (flat_ids[:, None] == jnp.arange(experts, dtype=jnp.int32)[None, :]).astype(jnp.int32)
    earlier = jnp.cumsum(onehot, axis=0) - onehot
    slot_index = jnp.sum(earlier * onehot, axis=1)
    target = flat_ids * capacity + slot_index
    row_owner = jnp.full((experts * capacity,), tok_rows, jnp.int32)
    row_owner = row_owner.at[target].set(
        jnp.arange(flat_ids.shape[0], dtype=jnp.int32) // top_count
    )
    half_width = model_width // tp_count
    source = lax.dynamic_slice_in_dim(tokens, lax.axis_index("tp") * half_width, half_width, 1)
    padded = jnp.concatenate([source, jnp.zeros((1, source.shape[1]), jnp.bfloat16)], axis=0)
    outgoing = jnp.take(padded, row_owner, axis=0).reshape(ep_count, capacity, source.shape[1])
    parted = lax.all_to_all(outgoing, "ep", split_axis=0, concat_axis=0, tiled=True)
    arrived = lax.all_gather(parted, "tp", axis=2, tiled=True)
    expert_rows = arrived.reshape(-1, model_width)
    partial_value = expert_apply(expert_rows, w_gate[0], w_up[0], w_down[0])
    shared = expert_apply(tokens, shared_gate, shared_up, shared_down)
    returned = lax.all_to_all(
        partial_value.reshape(ep_count, capacity, model_width).astype(jnp.bfloat16),
        "ep",
        split_axis=0,
        concat_axis=0,
        tiled=True,
    ).astype(jnp.float32)
    routed = combine_rows(returned, target, weights, tok_rows, top_count)
    return lax.psum_scatter(routed + shared, "tp", scatter_dimension=1, tiled=True).astype(
        jnp.bfloat16
    )


MESH = pl.DeviceIdType.MESH
LANES = 128
VMEM_BYTES = 66_000_000


def ring_order(position):
    return position + (position // 2 % 2) * (1 - 2 * (position % 2))


def fused_kernel(
    side, tok, tab, w_gate, w_up, w_down, s_gate, s_up, s_down, out,
    x, table, own, away, peer, hidden, gate_w, up_w, down_w,
    shared_own, shared_away, shared_peer, ring1, ring2,
    local_sem, arrive, cross, plane_recv, ring1_recv, ring2_recv, send_sem,
):
    rows = tok.shape[0]
    half_rows = rows // 2
    half = tok.shape[1] // 2
    part = half // 2
    fe = w_gate.shape[1]
    me = lax.axis_index("ep")
    core = lax.axis_index("tp")
    zpos = me // side
    ppos = ring_order(me % side)

    def block_of(p, z):
        return lax.rem(z + 2 * side, side) * side + ring_order(lax.rem(p + 2 * side, side))

    def neighbour(axis, step):
        if axis == 0:
            return {"ep": block_of(ppos + step, zpos)}
        return {"ep": block_of(ppos, zpos + step)}

    partner = {"tp": 1 - core}
    barrier = pltpu.get_barrier_semaphore()
    for axis in (0, 1):
        for step in (1, -1):
            pl.semaphore_signal(barrier, inc=1, device_id=neighbour(axis, step), device_id_type=MESH)
    pl.semaphore_signal(barrier, inc=1, device_id=partner, device_id_type=MESH)

    def load(sources):
        copies = []
        for number, (src, dst) in enumerate(zip(sources, (gate_w, up_w, down_w))):
            copy = pltpu.make_async_copy(src, dst, local_sem.at[number])
            copy.start()
            copies.append(copy)
        return copies

    mine = pltpu.make_async_copy(tok, x.at[pl.ds(pl.multiple_of(me * rows, rows), rows)], local_sem.at[3])
    mine_table = pltpu.make_async_copy(tab, table.at[me], local_sem.at[4])
    mine.start()
    mine_table.start()
    shared_copies = load((s_gate, s_up, s_down))
    mine.wait()
    mine_table.wait()
    pl.semaphore_wait(barrier, 5)

    pending = []

    def send(src, dst, recv_sem, device):
        copy = pltpu.make_async_remote_copy(
            src_ref=src, dst_ref=dst, send_sem=send_sem.at[len(pending)], recv_sem=recv_sem,
            device_id=device, device_id_type=MESH,
        )
        copy.start()
        pending.append(copy)

    def arrived(ref, recv_sem):
        pltpu.make_async_remote_copy(
            src_ref=ref, dst_ref=ref, send_sem=send_sem.at[0], recv_sem=recv_sem,
            device_id=partner, device_id_type=MESH,
        ).wait_recv()

    def piece(block, s, v, which):
        if s == 2:
            return table.at[block]
        column = pl.multiple_of(which * half + s * part, LANES)
        return x.at[pl.ds(pl.multiple_of(block * rows + v * half_rows, half_rows), half_rows), pl.ds(column, part)]

    def hops(v):
        ahead = side // 2 if v == 0 else (side - 1) // 2
        return ahead, side - 1 - ahead

    streams = [(0, 0), (1, 0), (0, 1), (1, 1), (2, 0)]

    def axes(s):
        return (1, 0) if s == 1 else (0, 1)

    def at(s, first, second):
        if axes(s)[0] == 0:
            return block_of(ppos + first, zpos + second)
        return block_of(ppos + second, zpos + first)

    def forward(s, v, first, second, axis, step):
        block = at(s, first, second)
        ref = piece(block, s, v, core)
        send(ref, ref, arrive.at[s, v, block], neighbour(axis, step))

    def receive(s, v, first, second):
        block = at(s, first, second)
        ref = piece(block, s, v, core)
        arrived(ref, arrive.at[s, v, block])
        if s < 2:
            send(ref, ref, cross.at[s, v, block], partner)

    def reach(v, step):
        ahead, back = hops(v)
        return ahead if step == 1 else back

    def fan(s, v, first):
        for step in (1, -1):
            if reach(v, step) >= 1:
                forward(s, v, first, 0, axes(s)[1], step)

    for s, v in streams:
        for step in (1, -1):
            if reach(v, step) >= 1:
                forward(s, v, 0, 0, axes(s)[0], step)
    for s, v in streams:
        fan(s, v, 0)
    longest = side // 2
    for k in range(1, longest + 1):
        for s, v in streams:
            for step in (1, -1):
                if k <= reach(v, step):
                    receive(s, v, -step * k, 0)
                    if k < reach(v, step):
                        forward(s, v, -step * k, 0, axes(s)[0], step)
                    fan(s, v, -step * k)

    firsts = [0]
    for k in range(1, longest + 1):
        firsts += [-k, k]
    firsts = firsts[:side]

    def second_phase(k, group):
        for first in group:
            for s, v in streams:
                for step in (1, -1):
                    if k <= reach(v, step):
                        position = first
                        receive(s, v, position, -step * k)
                        if k < reach(v, step):
                            forward(s, v, position, -step * k, axes(s)[1], step)

    def swiglu(inputs, columns):
        gate = jnp.dot(inputs, gate_w[:, columns], preferred_element_type=jnp.float32)
        up = jnp.dot(inputs, up_w[:, columns], preferred_element_type=jnp.float32)
        return gate / (1.0 + jnp.exp(-gate)) * up

    tile = 256
    for copy in shared_copies:
        copy.wait()

    @pl.loop(0, fe // tile)
    def _(j):
        columns = pl.ds(pl.multiple_of(j * tile, tile), tile)
        inputs = x[pl.ds(pl.multiple_of(me * rows, rows), rows), :]
        hidden[0:rows, columns] = swiglu(inputs, columns).astype(jnp.bfloat16)

    @pl.loop(0, half // tile)
    def _(j):
        columns = pl.ds(pl.multiple_of(j * tile, tile), tile)
        mine_columns = pl.ds(pl.multiple_of(core * half + j * tile, tile), tile)
        other_columns = pl.ds(pl.multiple_of((1 - core) * half + j * tile, tile), tile)
        h = hidden[0:rows, :]
        shared_own[:, columns] = jnp.dot(h, down_w[:, mine_columns], preferred_element_type=jnp.float32)
        shared_away[:, columns] = jnp.dot(h, down_w[:, other_columns], preferred_element_type=jnp.float32)

    send(shared_away, shared_peer, plane_recv.at[side], partner)
    expert_copies = load((w_gate, w_up, w_down))

    for k in range(1, longest + 1):
        second_phase(k, firsts)
    for block_step in range(1, side * side):
        block = lax.rem(me + block_step, side * side)
        for s in (0, 1):
            for v in (0, 1):
                arrived(piece(block, s, v, 1 - core), cross.at[s, v, block])
    for copy in expert_copies:
        copy.wait()

    group = 2 * rows

    def plane(offset):
        z = lax.rem(zpos + offset + side, side)

        @pl.loop(0, side // 2)
        def _(m):
            start = pl.multiple_of((z * side + 2 * m) * rows, group)
            columns_of = []
            for b in range(2):
                values = table[z * side + 2 * m + b]
                lines = lax.broadcasted_iota(jnp.int32, values.shape, 0)
                line = jnp.sum(jnp.where(lines == me, values, 0.0), axis=0, keepdims=True)
                columns_of.append(jnp.broadcast_to(line, (rows, rows)).T[:, :1])
            weight = jnp.concatenate(columns_of, axis=0)

            @pl.loop(0, fe // tile)
            def _(j):
                columns = pl.ds(pl.multiple_of(j * tile, tile), tile)
                value = swiglu(x[pl.ds(start, group), :], columns) * weight
                hidden[pl.ds(pl.multiple_of(m * group, group), group), columns] = value.astype(jnp.bfloat16)

        @pl.loop(0, half // tile)
        def _(j):
            columns = pl.ds(pl.multiple_of(j * tile, tile), tile)
            mine_columns = pl.ds(pl.multiple_of(core * half + j * tile, tile), tile)
            other_columns = pl.ds(pl.multiple_of((1 - core) * half + j * tile, tile), tile)
            h = hidden[...]
            value = jnp.dot(h, down_w[:, other_columns], preferred_element_type=jnp.float32)
            away[z, :, :, columns] = value.astype(jnp.bfloat16).reshape(side, rows, tile)
            value = jnp.dot(h, down_w[:, mine_columns], preferred_element_type=jnp.float32)
            own[z, :, :, columns] = value.astype(jnp.bfloat16).reshape(side, rows, tile)

        send(away.at[z], peer.at[z], plane_recv.at[z], partner)

    def join(offset):
        z = lax.rem(zpos + offset + side, side)
        arrived(peer.at[z], plane_recv.at[z])

        @pl.loop(0, side)
        def _(b):
            total = own[z, b].astype(jnp.float32) + peer[z, b].astype(jnp.float32)
            own[z, b] = total.astype(jnp.bfloat16)

    planes = [firsts[-1]] + firsts[1:-1] + [0] if side > 1 else [0]

    def own_piece(s, v, target, inner):
        spot = pl.ds(v * half_rows, half_rows), pl.ds(s * part, part)
        if s == 0:
            return (lax.rem(zpos + target + 2 * side, side), inner) + spot
        return (inner, ring_order(lax.rem(ppos + target + 2 * side, side))) + spot

    def slot_of(v, step, k):
        return k - 1 if step == 1 else reach(v, 1) + k - 1

    def add_into(s, v, target, slots):
        @pl.loop(0, side)
        def _(inner):
            index = own_piece(s, v, target, inner)
            total = own[index].astype(jnp.float32)
            for slot in slots:
                total += ring1[s, v, slot, inner].astype(jnp.float32)
            own[index] = total.astype(jnp.bfloat16)

    def ring1_step(s, v, step, k):
        target = step * (reach(v, step) - k + 1)
        if k > 1:
            slot = slot_of(v, step, k - 1)
            arrived(ring1.at[s, v, slot], ring1_recv.at[s, v, slot])
            add_into(s, v, target, [slot])
        slot = slot_of(v, step, k)
        source = own.at[own_piece(s, v, target, pl.ds(0, side))]
        send(source, ring1.at[s, v, slot], ring1_recv.at[s, v, slot], neighbour(1 - s, step))

    def same_plane(a, b):
        return (a - b) % side == 0

    done = []
    for number, offset in enumerate(planes):
        plane(offset)
        if number > 0:
            done.append(planes[number - 1])
            join(planes[number - 1])
            for v in (0, 1):
                for step in (1, -1):
                    if reach(v, step) >= 1 and same_plane(step * reach(v, step), planes[number - 1]):
                        ring1_step(0, v, step, 1)
    join(planes[-1])
    for v in (0, 1):
        for step in (1, -1):
            if reach(v, step) >= 1:
                ring1_step(1, v, step, 1)
    for k in range(2, longest + 1):
        for s in (0, 1):
            for v in (0, 1):
                for step in (1, -1):
                    if k <= reach(v, step):
                        ring1_step(s, v, step, k)

    def last_piece(s, v, target):
        spot = pl.ds(v * half_rows, half_rows), pl.ds(s * part, part)
        if s == 0:
            return (zpos, ring_order(lax.rem(ppos + target + 2 * side, side))) + spot
        return (lax.rem(zpos + target + 2 * side, side), ring_order(ppos)) + spot

    def ring2_step(s, v, step, k):
        target = step * (reach(v, step) - k + 1)
        index = last_piece(s, v, target)
        if k > 1:
            slot = slot_of(v, step, k - 1)
            arrived(ring2.at[s, v, slot], ring2_recv.at[s, v, slot])
            total = own[index].astype(jnp.float32) + ring2[s, v, slot].astype(jnp.float32)
            own[index] = total.astype(jnp.bfloat16)
        slot = slot_of(v, step, k)
        send(own.at[index], ring2.at[s, v, slot], ring2_recv.at[s, v, slot], neighbour(s, step))

    for s in (0, 1):
        for v in (0, 1):
            slots = []
            for step in (1, -1):
                if reach(v, step) >= 1:
                    slot = slot_of(v, step, reach(v, step))
                    arrived(ring1.at[s, v, slot], ring1_recv.at[s, v, slot])
                    slots.append(slot)
            add_into(s, v, 0, slots)
            for step in (1, -1):
                if reach(v, step) >= 1:
                    ring2_step(s, v, step, 1)
    for k in range(2, longest + 1):
        for s in (0, 1):
            for v in (0, 1):
                for step in (1, -1):
                    if k <= reach(v, step):
                        ring2_step(s, v, step, k)
    arrived(shared_peer, plane_recv.at[side])
    for s in (0, 1):
        for v in (0, 1):
            spot = pl.ds(v * half_rows, half_rows), pl.ds(s * part, part)
            total = own[last_piece(s, v, 0)].astype(jnp.float32)
            for step in (1, -1):
                if reach(v, step) >= 1:
                    slot = slot_of(v, step, reach(v, step))
                    arrived(ring2.at[s, v, slot], ring2_recv.at[s, v, slot])
                    total += ring2[s, v, slot].astype(jnp.float32)
            total += shared_own[spot] + shared_peer[spot]
            out[spot] = total.astype(jnp.bfloat16)
    for copy in pending:
        copy.wait_send()


def per_device_fused(
    side, tokens, expert_ids, gate_values, w_gate, w_up, w_down, shared_gate, shared_up, shared_down
):
    rows, width = tokens.shape
    n = side * side
    half, part = width // 2, width // 4
    fe = w_gate.shape[2]
    weights = route_scale * gate_values / jnp.sum(gate_values, axis=1, keepdims=True)
    chosen = expert_ids.T[:, None, :] == jnp.arange(n, dtype=jnp.int32)[None, :, None]
    tab = jnp.sum(jnp.where(chosen, weights.T[:, None, :], 0.0), axis=0)
    sends = 5 * (n - 1) + 4 * (n - 1) + 8 * (side - 1) + side + 1
    dma = pltpu.SemaphoreType.DMA
    bf, f32 = jnp.bfloat16, jnp.float32
    anywhere = pl.BlockSpec(memory_space=pl.ANY)
    return pl.pallas_call(
        functools.partial(fused_kernel, side),
        out_shape=jax.ShapeDtypeStruct((rows, half), bf),
        in_specs=[anywhere] * 8,
        out_specs=pl.BlockSpec(memory_space=pltpu.VMEM),
        scratch_shapes=[
            pltpu.VMEM((n * rows, width), bf),
            pltpu.VMEM((n, n, rows), f32),
            pltpu.VMEM((side, side, rows, half), bf),
            pltpu.VMEM((side, side, rows, half), bf),
            pltpu.VMEM((side, side, rows, half), bf),
            pltpu.VMEM((side * rows, fe), bf),
            pltpu.VMEM((width, fe), bf),
            pltpu.VMEM((width, fe), bf),
            pltpu.VMEM((fe, width), bf),
            pltpu.VMEM((rows, half), f32),
            pltpu.VMEM((rows, half), f32),
            pltpu.VMEM((rows, half), f32),
            pltpu.VMEM((2, 2, side - 1, side, rows // 2, part), bf),
            pltpu.VMEM((2, 2, side - 1, rows // 2, part), bf),
            dma((5,)),
            dma((3, 2, n)),
            dma((2, 2, n)),
            dma((side + 1,)),
            dma((2, 2, side - 1)),
            dma((2, 2, side - 1)),
            dma((sends,)),
        ],
        compiler_params=pltpu.CompilerParams(
            collective_id=0, has_side_effects=True, vmem_limit_bytes=VMEM_BYTES
        ),
    )(tokens, tab, w_gate[0], w_up[0], w_down[0], shared_gate, shared_up, shared_down)


def per_device(tokens, expert_ids, gate_values, w_gate, *rest):
    n, cores = lax.axis_size("ep"), lax.axis_size("tp")
    rows, width = tokens.shape
    side = math.isqrt(n)
    fe = w_gate.shape[2]
    needed = 2 * n * rows * width * 5 // 2 + 6 * fe * width + n * rows * width
    fits = side * side == n and side % 4 == 0 and cores == 2 and rows == LANES
    fits = fits and w_gate.shape[0] == 1 and rest[2].shape[1] == fe
    fits = fits and width % (4 * LANES) == 0 and width // 2 % 256 == 0 and fe % 256 == 0
    if fits and needed < VMEM_BYTES:
        return per_device_fused(side, tokens, expert_ids, gate_values, w_gate, *rest)
    return per_device_routed(tokens, expert_ids, gate_values, w_gate, *rest)


def solution(mesh):
    return jax.shard_map(
        per_device,
        mesh=mesh,
        in_specs=(
            P("ep", None),
            P("ep", None),
            P("ep", None),
            P("ep", None, "tp"),
            P("ep", None, "tp"),
            P("ep", "tp", None),
            P(None, "tp"),
            P(None, "tp"),
            P("tp", None),
        ),
        out_specs=P("ep", "tp"),
        check_vma=False,
    )
```
